32 devices in a mesh: leaf: 32 (over z, y, x, core).
Axes of the slice: x: 2, y: 2, z: 4, core: 2. Of those that a mesh axis runs over, the one named last changes fastest.
Arguments:
- coords: float32 [3, 262144], P(None, 'leaf'), may hold values from 0 to 1
- charges: bfloat16 [262144, 128], P('leaf'), may hold values from -6 to 6
- near_leaves: int32 [2048, 27], P('leaf'), may hold values from 0 to 191
- leaf_basis: bfloat16 [2048, 4096], P('leaf'), may hold values from -1 to 1
- leaf_transfer: bfloat16 [2048, 1024], P('leaf'), may hold values from -0.75 to 0.75
- mid_transfer: bfloat16 [256, 1024], P('leaf'), may hold values from -0.75 to 0.75
- base_transfer: bfloat16 [32, 1024], P('leaf'), may hold values from -0.75 to 0.75
- base_coupling: bfloat16 [6048, 1024], P('leaf'), may hold values from -0.01953125 to 0.01953125
- base_target: int32 [6048, 1], P('leaf'), may hold values from 0 to 31; in each aligned block of 189 rows (0 to 188, 189 to 377, ...) at most 11 rows name the same one
- base_source: int32 [6048], P('leaf'), may hold values from 0 to 31
- top_coupling: bfloat16 [256, 1024], P('leaf'), may hold values from -0.015625 to 0.015625
- top_target: int32 [256], P('leaf'), may hold values from 0 to 3
- top_source: int32 [256], P('leaf'), may hold values from 0 to 3
Outputs:
- potential: bfloat16 [262144, 128], P('leaf')
The draws below stay inside these ranges and needn't reach their ends.
Inputs may be any that keep to these rules, and one draw needn't show every extreme that they name: `near_leaves`: entry j of leaf l names leaf 64 * (l // 64 - 1) + j: a leaf of the device before in Morton order, of the row's own device, or of the device after; repeats may occur. `base_target`: among the 189 blocks of one device no base cluster is the target more than 11 times; that count is reached.
All inputs are finite; a program needn't handle non-finite values.
Results may differ from the reference program's by a relative error of at most 0.01.
Values may be sent and summed in bfloat16 or wider, within the bound.
A program may use at most 128 MiB of HBM per device.

```python
import math
import jax
import jax.numpy as jnp
import numpy as np
from jax import lax

K = 32
RHS = 128
M = 128
NNEAR = 27
NB = 189
TOPB_DEV = 8
LEAF_DEV = 64
BASE_DEV = 1
LEAVES = 2048
NPTS = 262144
MIDS = 256
NBASE = 32
NTOP = 4
BLK_DEV = 189
NBLK = 6048
NTBLK = 256
CAPC = 11
N_LEAF = 32


def set_ends(drawn, stream_key, smallest, top_value):
    shape = drawn.shape
    spot = [jax.random.randint(jax.random.fold_in(stream_key, axis), (), 0, shape[axis]) for axis in range(len(shape))]
    drawn = drawn.at[tuple(spot)].set(smallest)
    longest = shape.index(max(shape))
    spot[longest] = (spot[longest] + 1) % shape[longest]
    return drawn.at[tuple(spot)].set(top_value)


def shard_levels(rng, dims, pieces, smallest, high):
    loudness, own = 1.0, jax.random.fold_in(rng, 6)
    for position, blocks in pieces:
        draws = jnp.exp(jax.random.uniform(jax.random.fold_in(own, position), (blocks,), jnp.float32, smallest / len(pieces), high / len(pieces)))
        loudness = loudness * jnp.repeat(draws, dims[position] // blocks).reshape([-1 if axis == position else 1 for axis in range(len(dims))])
    return loudness


def shared_out(rng, own, number, rows, amount, top, bound, slope):
    ranking = jax.random.permutation(rng, amount)
    heavy_load, ordinary = shares(amount, rows * top, bound, slope, True), shares(amount, rows * top, bound, slope, False)
    places = jnp.arange(amount)

    def named(lengths, offset_by):
        used = int((lengths > 0).sum())
        fixed = max(1, used // 4)
        passed = fixed + (places - fixed + offset_by * (used - fixed)) % max(1, amount - fixed)
        return jnp.zeros((amount,), jnp.int32).at[ranking[jnp.where(places < fixed, places, passed)]].set(jnp.asarray(lengths, jnp.int32))

    lengths = jnp.where(number % 4 == 0, named(heavy_load, number // 4), named(ordinary, number - number // 4 - 1))
    mixed = jax.random.permutation(jax.random.fold_in(own, 3), amount)
    source_of, taker = mixed[0:amount // 2 * 2:2], mixed[1:amount // 2 * 2:2]
    margin = jnp.minimum(lengths[source_of] - 1, bound - lengths[taker]) // 2
    margin = jnp.where((source_of == ranking[0]) | (taker == ranking[0]) | (lengths[taker] == 0), 0, jnp.maximum(margin, 0))
    passed = jax.random.randint(jax.random.fold_in(own, 4), (amount // 2,), 0, 1 << 20) % (margin + 1)
    lengths = lengths.at[source_of].add(-passed).at[taker].add(passed)
    labels = jnp.searchsorted(jnp.cumsum(lengths), jnp.arange(rows * top), side="right").astype(jnp.int32)
    listing = labels.reshape(top, rows).T
    listing = listing[jax.random.permutation(jax.random.fold_in(own, 1), rows)]
    offset_by = jax.random.randint(jax.random.fold_in(own, 2), (rows, 1), 0, top)
    return jnp.take_along_axis(listing, (jnp.arange(top)[None, :] + offset_by) % top, axis=1)


def shares(count, total, bound, lean, full):
    weights = [(1 << 20) // math.isqrt(grade ** lean) + 1 for grade in range(1, count + 1)]
    largest = bound if full else min(bound, max(-(-total // count), total * weights[0] // sum(weights)))
    least = 1 if total - largest >= count - 1 else 0
    counts, spare = [largest] + [least] * (count - 1), total - largest - least * (count - 1)
    while spare > 0:
        movable = [i for i in range(1, count) if counts[i] < largest] or [i for i in range(1, count) if counts[i] < bound]
        whole, remaining = sum([weights[i] for i in movable]), spare
        for i in movable:
            more = min(bound - counts[i], max(1, remaining * weights[i] // whole), spare)
            counts[i] = counts[i] + more
            spare = spare - more
    return np.array(counts)


def centred(key, dims, spread, bound, pieces=(), kind=jnp.bfloat16):
    result = spread * jax.random.normal(key, dims, jnp.float32)
    if pieces:
        result = result * shard_levels(key, dims, pieces, -0.22, 0.18)
    return jnp.clip(result, -bound, bound).astype(kind)


def setup_inputs(seed: int = 0) -> dict:
    arg_keys = jax.random.split(jax.random.key(seed), 14)
    coords = jnp.clip(1.0 * jax.random.uniform(arg_keys[0], (3, NPTS), jnp.float32) ** shard_levels(arg_keys[0], (3, NPTS), ((1, 32),), -0.2, 0.2), 0.0, 1.0)
    charges = centred(arg_keys[1], (NPTS, RHS), 1.0, 6.0, ((0, 32),))
    near_leaves = set_ends(jax.random.randint(arg_keys[2], (LEAVES, NNEAR), 0, 3 * LEAF_DEV), jax.random.fold_in(arg_keys[2], 1), 0, (3 * LEAF_DEV) - 1).astype(jnp.int32)
    leaf_basis = centred(arg_keys[3], (LEAVES, K * M), K ** -0.5, 1.0, ((0, 32),))
    leaf_transfer = centred(arg_keys[4], (LEAVES, K * K), (2 * K) ** -0.5, 0.75, ((0, 32),))
    mid_transfer = centred(arg_keys[5], (MIDS, K * K), (2 * K) ** -0.5, 0.75, ((0, 32),))
    base_transfer = centred(arg_keys[6], (NBASE, K * K), (2 * K) ** -0.5, 0.75, ((0, 32),))
    base_coupling = centred(arg_keys[7], (NBLK, K * K), (16 * K * NB) ** -0.5, 0.01953125, ((0, 32),))
    base_target_keys = jax.random.split(jax.random.fold_in(arg_keys[8], 1), NBLK // BLK_DEV)
    base_target_turns = jax.random.permutation(jax.random.fold_in(arg_keys[8], 3), NBLK // BLK_DEV)
    base_target = jax.vmap(lambda own, number: shared_out(jax.random.fold_in(arg_keys[8], 2), own, number, BLK_DEV, NBASE, 1, CAPC, 1))(base_target_keys, base_target_turns).reshape((NBLK, 1))
    base_source = set_ends(jax.random.randint(arg_keys[9], (NBLK,), 0, NBASE), jax.random.fold_in(arg_keys[9], 1), 0, NBASE - 1).astype(jnp.int32)
    top_coupling = centred(arg_keys[10], (NTBLK, K * K), (512 * K * TOPB_DEV // BASE_DEV) ** -0.5, 0.015625, ((0, 32),))
    top_target = set_ends(jax.random.randint(arg_keys[11], (NTBLK,), 0, NTOP), jax.random.fold_in(arg_keys[11], 1), 0, NTOP - 1).astype(jnp.int32)
    top_source = set_ends(jax.random.randint(arg_keys[12], (NTBLK,), 0, NTOP), jax.random.fold_in(arg_keys[12], 1), 0, NTOP - 1).astype(jnp.int32)
    return {"coords": coords, "charges": charges, "near_leaves": near_leaves, "leaf_basis": leaf_basis, "leaf_transfer": leaf_transfer, "mid_transfer": mid_transfer, "base_transfer": base_transfer, "base_coupling": base_coupling, "base_target": base_target, "base_source": base_source, "top_coupling": top_coupling, "top_target": top_target, "top_source": top_source}


delta_sq = 0.0025

def rounded_values(values):
    return lax.optimization_barrier(values.astype(jnp.bfloat16))

def near_block(points, pool_points, pool_charges, columns):
    near_scale = 1.0 / math.sqrt(columns.shape[1] * points.shape[2])

    def near_step(running, column):
        other_points = jnp.take(pool_points, column, axis=1)
        other_charges = jnp.take(pool_charges, column, axis=0)
        squares = lax.optimization_barrier(jnp.sum((points[:, :, :, None] - other_points[:, :, None, :]) ** 2, axis=0))
        kernel = rounded_values(near_scale / jnp.sqrt(squares + delta_sq))
        update = jnp.einsum('lab,lbr->lar', kernel.astype(jnp.float32), other_charges.astype(jnp.float32))
        return (running + update, None)
    initial = jnp.zeros((points.shape[1], points.shape[2], pool_charges.shape[2]), jnp.float32)
    running, unused = lax.scan(near_step, initial, columns.T)
    return running

def reference(coords, charges, near_leaves, leaf_basis, leaf_transfer, mid_transfer, base_transfer, base_coupling, base_target, base_source, top_coupling, top_target, top_source):
    single_precision = jnp.float32
    charge_row_block = charges.reshape(LEAVES, M, RHS)
    basis_matrix = leaf_basis.reshape(LEAVES, K, M)
    leaf_coefficients = rounded_values(jnp.einsum('xpt,xtu->xpu', basis_matrix.astype(single_precision), charge_row_block.astype(single_precision)))
    mid_coeffs = rounded_values(jnp.einsum('mckp,mckr->mpr', leaf_transfer.reshape(MIDS, 8, K, K).astype(single_precision), leaf_coefficients.reshape(MIDS, 8, K, RHS).astype(single_precision)))
    base_coeffs = rounded_values(jnp.einsum('mckp,mckr->mpr', mid_transfer.reshape(NBASE, 8, K, K).astype(single_precision), mid_coeffs.reshape(NBASE, 8, K, RHS).astype(single_precision)))
    base_lift = base_transfer.reshape(NBASE, K, K)
    lifted = rounded_values(jnp.einsum('bkp,bkr->bpr', base_lift.astype(single_precision), base_coeffs.astype(single_precision)))
    top_coeffs = rounded_values(lax.optimization_barrier(jnp.sum(lifted.reshape(NTOP, 8, K, RHS).astype(single_precision), axis=1)))

    def add_portion(running, portion):
        blocks, targets, sources = portion
        products = jnp.einsum('bts,bsr->btr', blocks.reshape(-1, K, K).astype(single_precision), jnp.take(base_coeffs, sources, axis=0).astype(single_precision))
        return (running + jax.ops.segment_sum(products, targets, num_segments=NBASE), None)
    portions = (base_coupling.reshape(N_LEAF, BLK_DEV, K * K), base_target.reshape(N_LEAF, BLK_DEV), base_source.reshape(N_LEAF, BLK_DEV))
    coupled, unused = lax.scan(add_portion, jnp.zeros((NBASE, K, RHS), single_precision), portions)
    top_products = jnp.einsum('bts,bsr->btr', top_coupling.reshape(NTBLK, K, K).astype(single_precision), jnp.take(top_coeffs, top_source, axis=0).astype(single_precision))
    top_field = rounded_values(jax.ops.segment_sum(top_products, top_target, num_segments=NTOP))
    base_field = rounded_values(coupled + jnp.einsum('bkp,bpr->bkr', base_lift.astype(single_precision), jnp.repeat(top_field, 8, axis=0).astype(single_precision)))
    mid_field = rounded_values(jnp.einsum('mkp,mpr->mkr', mid_transfer.reshape(MIDS, K, K).astype(single_precision), jnp.repeat(base_field, 8, axis=0).astype(single_precision)))
    leaf_potential = rounded_values(jnp.einsum('lkp,lpr->lkr', leaf_transfer.reshape(LEAVES, K, K).astype(single_precision), jnp.repeat(mid_field, 8, axis=0).astype(single_precision)))
    all_points = coords.reshape(3, LEAVES, M)
    padded_points = jnp.pad(all_points, ((0, 0), (LEAF_DEV, LEAF_DEV), (0, 0)))
    padded_charges = jnp.pad(charge_row_block, ((LEAF_DEV, LEAF_DEV), (0, 0), (0, 0)))
    device_ids = jnp.arange(N_LEAF, dtype=jnp.int32)

    def device_block(portion):
        device, columns, local_expansion_basis, local_potential = portion
        first = (device * LEAF_DEV).astype(jnp.int32)
        points = lax.dynamic_slice_in_dim(all_points, first, LEAF_DEV, 1)
        pool_points = lax.dynamic_slice_in_dim(padded_points, first, 3 * LEAF_DEV, 1)
        pool_charges = lax.dynamic_slice_in_dim(padded_charges, first, 3 * LEAF_DEV, 0)
        near_field = near_block(points, pool_points, pool_charges, columns)
        distant_field = jnp.einsum('cbz,cbw->czw', local_expansion_basis.astype(single_precision), local_potential.astype(single_precision))
        return (near_field + distant_field).astype(jnp.bfloat16)
    inputs = (device_ids, near_leaves.reshape(N_LEAF, LEAF_DEV, NNEAR), basis_matrix.reshape(N_LEAF, LEAF_DEV, K, M), leaf_potential.reshape(N_LEAF, LEAF_DEV, K, RHS))
    potential = lax.map(device_block, inputs)
    return potential.reshape(NPTS, RHS)
```

```python
import functools
import math

import jax
import jax.numpy as jnp
from jax import lax
from jax.experimental import pallas as pl
from jax.experimental.pallas import tpu as pltpu
from jax.sharding import PartitionSpec as P

K = 32
RHS = 128
M = 128
FEATURES = 32
DELTA_SQ = 0.0025

F32 = jnp.float32
BF16 = jnp.bfloat16
VMEM = pl.BlockSpec(memory_space=pltpu.VMEM)
SMEM = pl.BlockSpec(memory_space=pltpu.SMEM)
ANY = pl.BlockSpec(memory_space=pl.ANY)


def dot(a, b):
    return jnp.dot(a, b, preferred_element_type=F32)


def dot_ta(a, b):
    return lax.dot_general(a, b, (((0,), (0,)), ((), ())), preferred_element_type=F32)


def rows(index, size):
    return pl.ds(pl.multiple_of(index * size, size), size)


def pieces(x):
    high = lax.reduce_precision(x, 8, 7)
    rest = x - high
    middle = lax.reduce_precision(rest, 8, 7)
    return high, middle, lax.reduce_precision(rest - middle, 8, 7)


def split_points(coords, scale):
    x = (coords - 0.5) * scale
    h, m, l = pieces(x)
    return h, m, l, jnp.sum(x * x, axis=0, keepdims=True)


def target_features(coords, scale):
    h, m, l, norm = split_points(coords, scale)
    nh, nm, nl = pieces(norm + DELTA_SQ * scale * scale)
    ones = jnp.ones_like(norm)
    zeros = jnp.zeros((FEATURES - 24, coords.shape[1]), F32)
    return jnp.concatenate([h, h, m, h, l, m, nh, nm, nl, ones, ones, ones, zeros], axis=0)


def source_features(coords, scale):
    h, m, l, norm = split_points(coords, scale)
    nh, nm, nl = pieces(norm)
    ones = jnp.ones_like(norm)
    zeros = jnp.zeros((FEATURES - 24, coords.shape[1]), F32)
    h, m, l = -2.0 * h, -2.0 * m, -2.0 * l
    return jnp.concatenate(
        [h, m, h, l, h, m, ones, ones, ones, nh, nm, nl, zeros], axis=0
    ).astype(BF16)


def up_kernel(leaves, basis_ref, charges_ref, leaf_t_ref, mid_t_ref, base_t_ref, out_ref, coeffs):
    def group(i, carry):
        for j in range(8):
            leaf = i * 8 + j
            coeffs[rows(leaf, K), :] = dot(
                basis_ref[rows(leaf, K), :], charges_ref[rows(leaf, M), :]
            ).astype(BF16)
        return carry

    lax.fori_loop(0, leaves // 8, group, 0)
    mids = []
    for m in range(leaves // 8):
        part = slice(m * 8 * K, (m + 1) * 8 * K)
        mids.append(dot_ta(leaf_t_ref[part, :], coeffs[part, :]).astype(BF16))
    base = dot_ta(mid_t_ref[...], jnp.concatenate(mids, axis=0)).astype(BF16)
    out_ref[:K, :] = base
    out_ref[K:, :] = dot_ta(base_t_ref[...], base).astype(BF16)


def couple_kernel(
    devices, blocks, top_blocks, step,
    target_ref, source_ref, top_target_ref, top_source_ref,
    blocks_ref, top_blocks_ref, all_ref, out_ref, sums, top_coeffs, top_sums,
):
    sums[...] = jnp.zeros_like(sums)
    top_sums[...] = jnp.zeros_like(top_sums)
    for t in range(devices // 8):
        total = jnp.zeros((K, RHS), F32)
        for j in range(8):
            first = (t * 8 + j) * 2 * K + K
            total = total + all_ref[first : first + K, :].astype(F32)
        top_coeffs[t * K : (t + 1) * K, :] = total.astype(BF16)

    def group(i, carry):
        products = []
        for j in range(step):
            b = i * step + j
            products.append(
                dot(blocks_ref[rows(b, K), :], all_ref[rows(source_ref[b] * 2, K), :])
            )
        for j in range(step):
            where = rows(target_ref[i * step + j], K)
            sums[where, :] = sums[where, :] + products[j]
        return carry

    lax.fori_loop(0, blocks // step, group, 0)
    products = [
        dot(top_blocks_ref[b * K : (b + 1) * K, :], top_coeffs[rows(top_source_ref[b], K), :])
        for b in range(top_blocks)
    ]
    for b in range(top_blocks):
        where = rows(top_target_ref[b], K)
        top_sums[where, :] = top_sums[where, :] + products[b]
    for d in range(devices):
        out_ref[d * 2 * K : d * 2 * K + K, :] = sums[d * K : (d + 1) * K, :].astype(BF16)
        t = d // 8
        out_ref[d * 2 * K + K : (d + 1) * 2 * K, :] = top_sums[t * K : (t + 1) * K, :].astype(BF16)


def near_kernel(
    devices, leaves, named,
    near_ref, target_ref, source_ref, before_ref, own_ref, after_ref, got_ref,
    basis_ref, leaf_t_ref, mid_t_ref, base_t_ref, out_ref,
    pool, fields, even, odd, sems,
):
    points = leaves * M
    copies = [
        pltpu.make_async_copy(ref, pool.at[pl.ds(i * points, points), :], sems.at[i])
        for i, ref in enumerate((before_ref, own_ref, after_ref))
    ]
    for copy in copies:
        copy.start()

    total = jnp.sum(got_ref[...].astype(F32).reshape(devices, 2 * K, RHS), axis=0)
    base = (total[:K] + dot(base_t_ref[...], total[K:].astype(BF16))).astype(BF16)
    mid = dot(mid_t_ref[...], base).astype(BF16)
    for m in range(leaves // 8):
        part = slice(m * 8 * K, (m + 1) * 8 * K)
        fields[part, :] = dot(leaf_t_ref[part, :], mid[m * K : (m + 1) * K, :]).astype(BF16)

    groups = [range(j, min(j + 2, named)) for j in range(0, named, 2)]

    def make(leaf, kernel):
        mine = target_ref[:, rows(leaf, M)].T.astype(BF16)
        for group in groups:
            theirs = jnp.concatenate(
                [source_ref[:, rows(near_ref[leaf, j], M)] for j in group], axis=1
            )
            squares = dot(mine, theirs)
            kernel[:, group[0] * M : (group[-1] + 1) * M] = lax.rsqrt(squares.astype(BF16))

    def use(leaf, kernel):
        total = dot_ta(basis_ref[rows(leaf, K), :], fields[rows(leaf, K), :])
        for group in groups:
            theirs = jnp.concatenate([pool[rows(near_ref[leaf, j], M), :] for j in group], axis=0)
            total = total + dot(kernel[:, group[0] * M : (group[-1] + 1) * M], theirs)
        out_ref[rows(leaf, M), :] = total.astype(BF16)

    make(0, even)
    for copy in copies:
        copy.wait()

    def pair(i, carry):
        make(2 * i + 1, odd)
        use(2 * i, even)
        make(jnp.minimum(2 * i + 2, leaves - 1), even)
        use(2 * i + 1, odd)
        return carry

    lax.fori_loop(0, leaves // 2, pair, 0)


def per_device(
    coords,
    charges,
    near_leaves,
    leaf_basis,
    leaf_transfer,
    mid_transfer,
    base_transfer,
    base_coupling,
    base_target,
    base_source,
    top_coupling,
    top_target,
    top_source,
):
    leaves, named = near_leaves.shape
    devices = lax.axis_size("leaf")
    blocks, top_blocks = base_coupling.shape[0], top_coupling.shape[0]
    scale = math.sqrt(named * M)
    up = [(i, i + 1) for i in range(devices - 1)]
    down = [(i + 1, i) for i in range(devices - 1)]
    points_before = lax.ppermute(coords, "leaf", up)
    points_after = lax.ppermute(coords, "leaf", down)
    charges_before = lax.ppermute(charges, "leaf", up)
    charges_after = lax.ppermute(charges, "leaf", down)

    basis = leaf_basis.reshape(-1, M)
    leaf_t = leaf_transfer.reshape(-1, K)
    mid_t = mid_transfer.reshape(-1, K)
    base_t = base_transfer.reshape(-1, K)
    limit = pltpu.CompilerParams(vmem_limit_bytes=48 * 1024 * 1024)

    mine = pl.pallas_call(
        functools.partial(up_kernel, leaves),
        out_shape=jax.ShapeDtypeStruct((2 * K, RHS), BF16),
        in_specs=[VMEM] * 5,
        out_specs=VMEM,
        scratch_shapes=[pltpu.VMEM((leaves * K, RHS), BF16)],
        compiler_params=limit,
        cost_estimate=pl.CostEstimate(flops=70_000_000, bytes_accessed=3_000_000, transcendentals=0),
        name="upward",
    )(basis, charges, leaf_t, mid_t, base_t)
    gathered = lax.all_gather(mine, "leaf", axis=0, tiled=True)

    step = max(s for s in range(1, 33) if blocks % s == 0)
    partial = pl.pallas_call(
        functools.partial(couple_kernel, devices, blocks, top_blocks, step),
        out_shape=jax.ShapeDtypeStruct((devices * 2 * K, RHS), BF16),
        in_specs=[SMEM] * 4 + [VMEM] * 3,
        out_specs=VMEM,
        scratch_shapes=[
            pltpu.VMEM((devices * K, RHS), F32),
            pltpu.VMEM((devices // 8 * K, RHS), BF16),
            pltpu.VMEM((devices // 8 * K, RHS), F32),
        ],
        compiler_params=limit,
        cost_estimate=pl.CostEstimate(flops=50_000_000, bytes_accessed=3_000_000, transcendentals=0),
        name="couple",
    )(
        base_target[:, 0], base_source, top_target, top_source,
        base_coupling.reshape(-1, K), top_coupling.reshape(-1, K), gathered,
    )
    got = lax.all_to_all(partial, "leaf", split_axis=0, concat_axis=0, tiled=True)

    targets = target_features(coords, scale)
    sources = source_features(
        jnp.concatenate([points_before, coords, points_after], axis=1), scale
    )
    return pl.pallas_call(
        functools.partial(near_kernel, devices, leaves, named),
        out_shape=jax.ShapeDtypeStruct((leaves * M, RHS), BF16),
        in_specs=[SMEM, VMEM, VMEM, ANY, ANY, ANY] + [VMEM] * 5,
        out_specs=VMEM,
        scratch_shapes=[
            pltpu.VMEM((3 * leaves * M, RHS), BF16),
            pltpu.VMEM((leaves * K, RHS), BF16),
            pltpu.VMEM((M, named * M), BF16),
            pltpu.VMEM((M, named * M), BF16),
            pltpu.SemaphoreType.DMA((3,)),
        ],
        compiler_params=limit,
        cost_estimate=pl.CostEstimate(
            flops=8_000_000_000, bytes_accessed=12_000_000, transcendentals=28_000_000
        ),
        name="near",
    )(
        near_leaves, targets, sources, charges_before, charges, charges_after, got,
        basis, leaf_t, mid_t, base_t,
    )


def solution(mesh):
    split, flat = P("leaf", None), P("leaf")
    in_specs = (P(None, "leaf"),) + (split,) * 8 + (flat, split, flat, flat)
    return jax.shard_map(
        per_device, mesh=mesh, in_specs=in_specs, out_specs=split, check_vma=False
    )
```

```python
import functools
import math

import jax
import jax.numpy as jnp
from jax import lax
from jax.experimental import pallas as pl
from jax.experimental.pallas import tpu as pltpu
from jax.sharding import PartitionSpec as P

K = 32
RHS = 128
M = 128
FEATURES = 32
DELTA_SQ = 0.0025

F32 = jnp.float32
BF16 = jnp.bfloat16
VMEM = pl.BlockSpec(memory_space=pltpu.VMEM)
SMEM = pl.BlockSpec(memory_space=pltpu.SMEM)
ANY = pl.BlockSpec(memory_space=pl.ANY)


def dot(a, b):
    return jnp.dot(a, b, preferred_element_type=F32)


def dot_ta(a, b):
    return lax.dot_general(a, b, (((0,), (0,)), ((), ())), preferred_element_type=F32)


def rows(index, size):
    return pl.ds(pl.multiple_of(index * size, size), size)


def pieces(x):
    high = x.astype(BF16).astype(F32)
    rest = x - high
    middle = rest.astype(BF16).astype(F32)
    return high, middle, (rest - middle).astype(BF16).astype(F32)


def write_features(rows_ref, first, width, parts):
    at = 0
    for part in parts:
        rows_ref[at : at + part.shape[0], pl.ds(first, width)] = part
        at += part.shape[0]


def up_kernel(leaves, basis_ref, charges_ref, leaf_t_ref, mid_t_ref, base_t_ref, out_ref, coeffs):
    def group(i, carry):
        for j in range(8):
            leaf = i * 8 + j
            coeffs[rows(leaf, K), :] = dot(
                basis_ref[rows(leaf, K), :], charges_ref[rows(leaf, M), :]
            ).astype(BF16)
        return carry

    lax.fori_loop(0, leaves // 8, group, 0)
    mids = []
    for m in range(leaves // 8):
        part = slice(m * 8 * K, (m + 1) * 8 * K)
        mids.append(dot_ta(leaf_t_ref[part, :], coeffs[part, :]).astype(BF16))
    base = dot_ta(mid_t_ref[...], jnp.concatenate(mids, axis=0)).astype(BF16)
    out_ref[:K, :] = base
    out_ref[K:, :] = dot_ta(base_t_ref[...], base).astype(BF16)


def couple_kernel(
    devices, blocks, top_blocks, step,
    target_ref, source_ref, top_target_ref, top_source_ref,
    blocks_ref, top_blocks_ref, all_ref, out_ref, sums, top_coeffs, top_sums,
):
    sums[...] = jnp.zeros_like(sums)
    top_sums[...] = jnp.zeros_like(top_sums)
    for t in range(devices // 8):
        total = jnp.zeros((K, RHS), F32)
        for j in range(8):
            first = (t * 8 + j) * 2 * K + K
            total = total + all_ref[first : first + K, :].astype(F32)
        top_coeffs[t * K : (t + 1) * K, :] = total.astype(BF16)

    def group(i, carry):
        products = []
        for j in range(step):
            b = i * step + j
            products.append(
                dot(blocks_ref[rows(b, K), :], all_ref[rows(source_ref[b] * 2, K), :])
            )
        for j in range(step):
            where = rows(target_ref[i * step + j], K)
            sums[where, :] = sums[where, :] + products[j]
        return carry

    lax.fori_loop(0, blocks // step, group, 0)
    products = [
        dot(top_blocks_ref[b * K : (b + 1) * K, :], top_coeffs[rows(top_source_ref[b], K), :])
        for b in range(top_blocks)
    ]
    for b in range(top_blocks):
        where = rows(top_target_ref[b], K)
        top_sums[where, :] = top_sums[where, :] + products[b]
    for d in range(devices):
        out_ref[d * 2 * K : d * 2 * K + K, :] = sums[d * K : (d + 1) * K, :].astype(BF16)
        t = d // 8
        out_ref[d * 2 * K + K : (d + 1) * 2 * K, :] = top_sums[t * K : (t + 1) * K, :].astype(BF16)


def groups_of(named):
    return [range(j, min(j + 2, named)) for j in range(0, named, 2)]


def make_kernel(
    leaves, named, scale, width,
    near_ref, before_ref, own_ref, after_ref, out_ref, targets, staged, sources,
):
    points = leaves * M

    @pl.when(pl.program_id(0) == 0)
    def _():
        for place, ref in enumerate((before_ref, own_ref, after_ref)):

            def chunk(i, carry, place=place, ref=ref):
                first = pl.multiple_of(i * width, width)
                x = (ref[:, pl.ds(first, width)] - 0.5) * scale
                h, m, l = pieces(x)
                norm = x[0:1] * x[0:1] + x[1:2] * x[1:2] + x[2:3] * x[2:3]
                ones = jnp.ones((3, width), F32)
                zeros = jnp.zeros((FEATURES - 24, width), F32)
                if place == 1:
                    n = pieces(norm + DELTA_SQ * scale * scale)
                    write_features(targets, first, width, [h, h, m, h, l, m, *n, ones, zeros])
                n = pieces(norm)
                h, m, l = -2.0 * h, -2.0 * m, -2.0 * l
                write_features(staged, 0, width, [h, m, h, l, h, m, ones, *n, zeros])
                where = pl.ds(pl.multiple_of(place * points + first, width), width)
                sources[:, where] = staged[...].astype(BF16)
                return carry

            lax.fori_loop(0, points // width, chunk, 0)

    for k in range(out_ref.shape[0]):
        leaf = pl.program_id(0) * out_ref.shape[0] + k
        mine = targets[:, rows(leaf, M)].T.astype(BF16)
        for group in groups_of(named):
            theirs = jnp.concatenate(
                [sources[:, rows(near_ref[leaf, j], M)] for j in group], axis=1
            )
            squares = dot(mine, theirs)
            out_ref[k, :, group[0] * M : (group[-1] + 1) * M] = lax.rsqrt(squares.astype(BF16))


def use_kernel(
    devices, leaves, named,
    near_ref, kernel_ref, before_ref, own_ref, after_ref, got_ref,
    basis_ref, leaf_t_ref, mid_t_ref, base_t_ref, out_ref,
    pool, fields, sems,
):
    points = leaves * M

    @pl.when(pl.program_id(0) == 0)
    def _():
        copies = [
            pltpu.make_async_copy(ref, pool.at[pl.ds(i * points, points), :], sems.at[i])
            for i, ref in enumerate((before_ref, own_ref, after_ref))
        ]
        for copy in copies:
            copy.start()
        total = jnp.sum(got_ref[...].astype(F32).reshape(devices, 2 * K, RHS), axis=0)
        base = (total[:K] + dot(base_t_ref[...], total[K:].astype(BF16))).astype(BF16)
        mid = dot(mid_t_ref[...], base).astype(BF16)
        for m in range(leaves // 8):
            part = slice(m * 8 * K, (m + 1) * 8 * K)
            fields[part, :] = dot(leaf_t_ref[part, :], mid[m * K : (m + 1) * K, :]).astype(BF16)
        for copy in copies:
            copy.wait()

    for k in range(kernel_ref.shape[0]):
        leaf = pl.program_id(0) * kernel_ref.shape[0] + k
        total = dot_ta(basis_ref[rows(leaf, K), :], fields[rows(leaf, K), :])
        for group in groups_of(named):
            theirs = jnp.concatenate([pool[rows(near_ref[leaf, j], M), :] for j in group], axis=0)
            total = total + dot(kernel_ref[k, :, group[0] * M : (group[-1] + 1) * M], theirs)
        out_ref[k * M : (k + 1) * M, :] = total.astype(BF16)


def per_device(
    coords,
    charges,
    near_leaves,
    leaf_basis,
    leaf_transfer,
    mid_transfer,
    base_transfer,
    base_coupling,
    base_target,
    base_source,
    top_coupling,
    top_target,
    top_source,
):
    leaves, named = near_leaves.shape
    devices = lax.axis_size("leaf")
    blocks, top_blocks = base_coupling.shape[0], top_coupling.shape[0]
    scale = math.sqrt(named * M)
    up = [(i, i + 1) for i in range(devices - 1)]
    down = [(i + 1, i) for i in range(devices - 1)]
    points_before = lax.ppermute(coords, "leaf", up)
    points_after = lax.ppermute(coords, "leaf", down)

    basis = leaf_basis.reshape(-1, M)
    leaf_t = leaf_transfer.reshape(-1, K)
    mid_t = mid_transfer.reshape(-1, K)
    base_t = base_transfer.reshape(-1, K)
    limit = pltpu.CompilerParams(vmem_limit_bytes=48 * 1024 * 1024)

    mine = pl.pallas_call(
        functools.partial(up_kernel, leaves),
        out_shape=jax.ShapeDtypeStruct((2 * K, RHS), BF16),
        in_specs=[VMEM] * 5,
        out_specs=VMEM,
        scratch_shapes=[pltpu.VMEM((leaves * K, RHS), BF16)],
        compiler_params=limit,
        cost_estimate=pl.CostEstimate(flops=70_000_000, bytes_accessed=3_000_000, transcendentals=0),
        name="upward",
    )(basis, charges, leaf_t, mid_t, base_t)
    gathered = lax.all_gather(mine, "leaf", axis=0, tiled=True)
    gathered, outgoing, points_before, points_after = lax.optimization_barrier(
        (gathered, charges, points_before, points_after)
    )
    charges_before = lax.ppermute(outgoing, "leaf", up)
    charges_after = lax.ppermute(outgoing, "leaf", down)

    step = max(s for s in range(1, 33) if blocks % s == 0)
    partial = pl.pallas_call(
        functools.partial(couple_kernel, devices, blocks, top_blocks, step),
        out_shape=jax.ShapeDtypeStruct((devices * 2 * K, RHS), BF16),
        in_specs=[SMEM] * 4 + [VMEM] * 3,
        out_specs=VMEM,
        scratch_shapes=[
            pltpu.VMEM((devices * K, RHS), F32),
            pltpu.VMEM((devices // 8 * K, RHS), BF16),
            pltpu.VMEM((devices // 8 * K, RHS), F32),
        ],
        compiler_params=limit,
        cost_estimate=pl.CostEstimate(flops=50_000_000, bytes_accessed=3_000_000, transcendentals=0),
        name="couple",
    )(
        base_target[:, 0], base_source, top_target, top_source,
        base_coupling.reshape(-1, K), top_coupling.reshape(-1, K), gathered,
    )
    got = lax.all_to_all(partial, "leaf", split_axis=0, concat_axis=0, tiled=True)

    partial, points_before = lax.optimization_barrier((partial, points_before))
    got = lax.all_to_all(partial, "leaf", split_axis=0, concat_axis=0, tiled=True)
    each = 4
    kernels = pl.pallas_call(
        functools.partial(make_kernel, leaves, named, scale, 1024),
        grid=(leaves // each,),
        out_shape=jax.ShapeDtypeStruct((leaves, M, named * M), BF16),
        in_specs=[SMEM, VMEM, VMEM, VMEM],
        out_specs=pl.BlockSpec((each, M, named * M), lambda i: (i, 0, 0)),
        scratch_shapes=[
            pltpu.VMEM((FEATURES, leaves * M), F32),
            pltpu.VMEM((FEATURES, 1024), F32),
            pltpu.VMEM((FEATURES, 3 * leaves * M), BF16),
        ],
        compiler_params=limit,
        cost_estimate=pl.CostEstimate(
            flops=16_000_000_000, bytes_accessed=60_000_000, transcendentals=28_000_000
        ),
        name="make",
    )(near_leaves, points_before, coords, points_after)
    return pl.pallas_call(
        functools.partial(use_kernel, devices, leaves, named),
        grid=(leaves // each,),
        out_shape=jax.ShapeDtypeStruct((leaves * M, RHS), BF16),
        in_specs=[SMEM, pl.BlockSpec((each, M, named * M), lambda i: (i, 0, 0)), ANY, ANY, ANY]
        + [VMEM] * 5,
        out_specs=pl.BlockSpec((each * M, RHS), lambda i: (i, 0)),
        scratch_shapes=[
            pltpu.VMEM((3 * leaves * M, RHS), BF16),
            pltpu.VMEM((leaves * K, RHS), BF16),
            pltpu.SemaphoreType.DMA((3,)),
        ],
        compiler_params=limit,
        cost_estimate=pl.CostEstimate(
            flops=8_000_000_000, bytes_accessed=66_000_000, transcendentals=0
        ),
        name="use",
    )(
        near_leaves, kernels, charges_before, charges, charges_after, got,
        basis, leaf_t, mid_t, base_t,
    )


def solution(mesh):
    split, flat = P("leaf", None), P("leaf")
    in_specs = (P(None, "leaf"),) + (split,) * 8 + (flat, split, flat, flat)
    return jax.shard_map(
        per_device, mesh=mesh, in_specs=in_specs, out_specs=split, check_vma=False
    )
```
